32 devices in a mesh: dp: 8 (over z, x), mp: 4 (over y, core).
Axes of the slice: x: 2, y: 2, z: 4, core: 2. Of those that a mesh axis runs over, the one named last changes fastest.
Arguments:
- teacher_states: bfloat16 [512, 128, 4096], P('dp', None, 'mp'), may hold values from -6 to 6
- teacher_gain: float32 [4096], P('mp'), may hold values from 0.25 to 1.75
- teacher_proj: bfloat16 [4096, 1024], P('mp'), may hold values from -0.09375 to 0.09375
- teacher_mask: int32 [512, 128], P('dp'), may hold values 0 or 1
- student_states: bfloat16 [1024, 64, 768], P(('dp', 'mp')), may hold values from -6 to 6
- student_gain: float32 [768], replicated, may hold values from 0.25 to 1.75
- student_proj: bfloat16 [768, 1024], replicated, may hold values from -0.21875 to 0.21875
- student_mask: int32 [1024, 64], P(('dp', 'mp')), may hold values 0 or 1
- positive: int32 [1024], P(('dp', 'mp')), may hold values from 0 to 511
Outputs:
- grad_embed: float32 [1024, 1024], P(('dp', 'mp'))
- grad_states: bfloat16 [1024, 64, 768], P(('dp', 'mp'))
The draws below stay inside these ranges and needn't reach their ends.
All inputs are finite; a program needn't handle non-finite values. No bound on the sum of `teacher_mask` or of `student_mask` on one device may be relied on, other than what follows from the above.
Results may differ from the reference program's by a relative error of at most 0.0085.
Values may be sent and summed in bfloat16 or wider, within the bound.
A program may use at most 128 MiB of HBM per device.

```python
import jax
import jax.numpy as jnp
from jax import lax

D = 4096
E = 1024
DS = 768
LEN = 128
QLEN = 64
PASSAGES = 512
QUERIES = 1024


def place_ends(result, rng, least, high):
    longest = result.shape.index(max(result.shape))
    spots = []
    for shift in (0, 1):
        where = [jax.random.randint(jax.random.fold_in(rng, axis), (), 0, length) for axis, length in enumerate(result.shape)]
        where[longest] = (where[longest] + shift) % result.shape[longest]
        spots.append(tuple(where))
    return result.at[spots[0]].set(least).at[spots[1]].set(high)


def block_scale(own_key, shape, cuts, least, top_value):
    def one(dim, shards_of):
        heights = jax.random.uniform(jax.random.fold_in(jax.random.fold_in(own_key, 6), dim), (shards_of,), jnp.float32, least / len(cuts), top_value / len(cuts))
        return jnp.repeat(jnp.exp(heights), shape[dim] // shards_of).reshape((-1,) + (1,) * (len(shape) - dim - 1))

    level = one(*cuts[0])
    for cut in cuts[1:]:
        level = level * one(*cut)
    return level


def normal_values(rng, shape, spread, reach, cuts=(), kind=jnp.bfloat16):
    drawn = spread * jax.random.normal(rng, shape, jnp.float32)
    if cuts:
        drawn = drawn * block_scale(rng, shape, cuts, -0.22, 0.18)
    return jnp.clip(drawn, -reach, reach).astype(kind)


def setup_inputs(seed: int = 0) -> dict:
    streams_of = jax.random.split(jax.random.key(seed), 10)
    teacher_states = normal_values(streams_of[0], (PASSAGES, LEN, D), 1.0, 6.0, ((0, 8), (2, 4)))
    teacher_gain = jnp.clip(1.0 + 0.15 * jax.random.normal(streams_of[1], (D,), jnp.float32), 0.25, 1.75)
    teacher_proj = normal_values(streams_of[2], (D, E), D ** -0.5, 0.09375, ((0, 4),))
    teacher_mask = place_ends((jax.random.randint(streams_of[3], (PASSAGES, LEN), 0, 4) < 3).astype(jnp.int32), jax.random.fold_in(streams_of[3], 1), 0, 1)
    student_states = normal_values(streams_of[4], (QUERIES, QLEN, DS), 1.0, 6.0, ((0, 32),))
    student_gain = jnp.clip(1.0 + 0.15 * jax.random.normal(streams_of[5], (DS,), jnp.float32), 0.25, 1.75)
    student_proj = normal_values(streams_of[6], (DS, E), DS ** -0.5, 0.21875)
    student_mask = place_ends((jax.random.randint(streams_of[7], (QUERIES, QLEN), 0, 4) < 3).astype(jnp.int32), jax.random.fold_in(streams_of[7], 1), 0, 1)
    positive = place_ends(jax.random.randint(streams_of[8], (QUERIES,), 0, PASSAGES), jax.random.fold_in(streams_of[8], 1), 0, PASSAGES - 1).astype(jnp.int32)
    return dict(teacher_states=teacher_states, teacher_gain=teacher_gain, teacher_proj=teacher_proj, teacher_mask=teacher_mask, student_states=student_states, student_gain=student_gain, student_proj=student_proj, student_mask=student_mask, positive=positive)


def pool_block(pair):
    states, live_mask = pair
    values = states.astype(jnp.float32)
    scale = lax.rsqrt(lax.optimization_barrier(jnp.mean(values * values, axis=-1)) + 1e-06)
    live = live_mask.astype(jnp.float32)
    weight = live * scale
    return lax.optimization_barrier(jnp.sum(values * weight[:, :, None], axis=1))

def unit_rows(values):
    return values * lax.rsqrt(lax.optimization_barrier(jnp.mean(values * values, axis=-1, keepdims=True)) + 1e-06) / jnp.sqrt(jnp.float32(values.shape[-1]))

def student_forward(states, gain, proj, live_mask):
    values = states.astype(jnp.float32)
    scale = lax.rsqrt(lax.optimization_barrier(jnp.mean(values * values, axis=-1, keepdims=True)) + 1e-06)
    normed = (values * scale * gain).astype(jnp.bfloat16)
    flat = normed.reshape(-1, normed.shape[-1])
    act = jax.nn.gelu(jnp.dot(flat, proj, preferred_element_type=jnp.float32), approximate=True)
    act = act.reshape(states.shape[0], states.shape[1], -1)
    live = live_mask.astype(jnp.float32)
    pooled = lax.optimization_barrier(jnp.sum(act * live[:, :, None], axis=1))
    return unit_rows(pooled)

def reference(teacher_states, teacher_gain, teacher_proj, teacher_mask, student_states, student_gain, student_proj, student_mask, positive):
    blocks = teacher_states.reshape(-1, 16, LEN, D)
    masks = teacher_mask.reshape(-1, 16, LEN)
    pooled = lax.map(pool_block, (blocks, masks)).reshape(PASSAGES, D)
    tpooled = (pooled * teacher_gain).astype(jnp.bfloat16)
    traw = jnp.dot(tpooled, teacher_proj, preferred_element_type=jnp.float32)
    temb = unit_rows(traw).astype(jnp.bfloat16)
    semb, back = jax.vjp(lambda st: student_forward(st, student_gain, student_proj, student_mask), student_states)
    sround = semb.astype(jnp.bfloat16)
    tpos = temb[positive]
    tlogit = 10.0 * jnp.dot(tpos, temb.T, preferred_element_type=jnp.float32)
    slogit = 20.0 * jnp.dot(sround, temb.T, preferred_element_type=jnp.float32)
    texp = jnp.exp(tlogit)
    sexp = jnp.exp(slogit)
    diff = (sexp / lax.optimization_barrier(jnp.sum(sexp, axis=1, keepdims=True)) - texp / lax.optimization_barrier(jnp.sum(texp, axis=1, keepdims=True))).astype(jnp.bfloat16)
    grad_embed = 20.0 * jnp.dot(diff, temb, preferred_element_type=jnp.float32)
    grad_states = back(grad_embed)[0]
    return (grad_embed, grad_states.astype(jnp.bfloat16))
```

```python
import functools

import jax
import jax.numpy as jnp
from jax import lax
from jax.experimental import pallas as pl
from jax.experimental.pallas import tpu as pltpu
from jax.sharding import PartitionSpec as P

MESH = pl.DeviceIdType.MESH
F32 = jnp.float32
BF16 = jnp.bfloat16
GROUPS = 4
ROOT = 0.7978845608028654
CUBE = 0.044715
LANES = 128
TILE = 256
NT = (((1,), (1,)), ((), ()))


def nearest(count):
    order = []
    for step in range(1, count // 2 + 1):
        order.append(step)
        if count - step != step:
            order.append(count - step)
    return order


def front(
    dn, n, ts, tmask, tgain, tproj, ss, sgain, sproj, smask, pos,
    ge_out, grad_out, h_out, x_out, scl_out, wt_out,
    tx, tp, sp, sw, live_col, sq, sqr, tpool, pf, pb, pr, te, raw_out, ua, ub,
    sem_tx, sem_in, sq_send, sq_recv, rs_send, rs_recv, dp_send, dp_recv, col_send, col_recv, fw_send, fw_recv,
):
    passages, length, feats = tx.shape
    width = n * feats
    rows = passages // n
    embed = tp.shape[1]
    chunks = passages // 8
    queries, qlen = smask.shape
    ds = sp.shape[0]
    tokens = TILE
    per_tile = tokens // qlen
    bodies = queries // (2 * per_tile)
    me_d, me_m = lax.axis_index("dp"), lax.axis_index("mp")
    half = n // 2
    core, chip = lax.rem(me_m, 2), me_m // 2

    def mp_peer(o):
        return (me_d, lax.rem(me_m + o, n))

    def dp_peer(o):
        return (lax.rem(me_d + o, dn), me_m)

    def col_peer(p):
        return (me_d, 2 * lax.rem(chip + p, half) + core)

    partner = (me_d, me_m + 1 - 2 * core)

    def load(c):
        part = pl.ds(c * 8, 8)
        return pltpu.make_async_copy(ts.at[part], tx.at[part], sem_tx.at[c])

    others = [
        pltpu.make_async_copy(sproj, sp, sem_in.at[0]),
        pltpu.make_async_copy(tproj, tp, sem_in.at[1]),
        pltpu.make_async_copy(ss, x_out, sem_in.at[2]),
    ]
    ahead = min(4, chunks)
    for c in range(ahead):
        load(c).start()
    barrier = pltpu.get_barrier_semaphore()
    for o in range(1, n):
        pl.semaphore_signal(barrier, inc=1, device_id=mp_peer(o), device_id_type=MESH)
    for o in range(1, dn):
        pl.semaphore_signal(barrier, inc=1, device_id=dp_peer(o), device_id_type=MESH)

    def remote(src, dst, send, recv, peer):
        return pltpu.make_async_remote_copy(
            src_ref=src, dst_ref=dst, send_sem=send, recv_sem=recv, device_id=peer, device_id_type=MESH
        )

    turned = jnp.transpose(smask[...].astype(F32))
    for q in range(queries):
        live_col[q * qlen : (q + 1) * qlen, :] = jnp.broadcast_to(turned[:, q : q + 1], (qlen, LANES))

    ones = jnp.ones((16, LANES), BF16)
    row8 = lax.broadcasted_iota(jnp.int32, (8, length), 0)
    row16 = lax.rem(lax.broadcasted_iota(jnp.int32, (16, length), 0), 8)
    per = chunks // GROUPS
    sq_copies = []

    def squares(c, carry):
        load(c).wait()

        @pl.when(c + ahead < chunks)
        def _():
            load(c + ahead).start()

        held = jnp.zeros((8, length), F32)
        for j in range(8):
            terms = []
            for k in range(feats // LANES):
                x = tx[c * 8 + j, :, k * LANES : (k + 1) * LANES]
                terms.append(x * x)
            while len(terms) > 1:
                terms = [a + b for a, b in zip(terms[::2], terms[1::2])] + terms[len(terms) // 2 * 2 :]
            line = lax.dot_general(ones, terms[0], NT, preferred_element_type=F32)
            held = jnp.where(row8 == j, line[:8], held)
        sq[c] = held
        return carry

    def send_squares(g):
        part = pl.ds(g * per, per)
        for o in range(1, n):
            copy = remote(sq.at[part], sqr.at[o, part], sq_send.at[o, g], sq_recv.at[o, g], mp_peer(o))
            copy.start()
            sq_copies.append(copy)

    def pool(c, carry):
        total = sq[c]
        for o in range(1, n):
            total = total + sqr[o, c]
        part = pl.ds(pl.multiple_of(c * 8, 8), 8)
        weight = tmask[part, :].astype(F32) * lax.rsqrt(total / width + 1e-06)
        high = weight.astype(BF16).astype(F32)
        both = jnp.concatenate([high, weight - high], axis=0)
        left = jnp.concatenate([jnp.where(row16 == j, both, 0.0) for j in range(8)], axis=1).astype(BF16)
        sums = jnp.dot(left, tx[pl.ds(c * 8, 8)].reshape(8 * length, feats), preferred_element_type=F32)
        tpool[part, :] = (sums[:8] + sums[8:]) * tgain[...].reshape(1, feats)
        return carry

    def pooling(g):
        for o in range(1, n):
            sq_copies[g * (n - 1) + o - 1].wait_recv()
        lax.fori_loop(g * per, (g + 1) * per, pool, 0)

    lax.fori_loop(0, 2 * per, squares, 0)
    pl.semaphore_wait(barrier, n + dn - 2)
    for copy in others:
        copy.start()
    send_squares(0)
    send_squares(1)
    lax.fori_loop(2 * per, 3 * per, squares, 0)
    send_squares(2)
    lax.fori_loop(3 * per, 4 * per, squares, 0)
    send_squares(3)
    pooling(0)
    pooling(1)
    pooling(2)

    others[0].wait()
    gain_col = jnp.transpose(jnp.broadcast_to(sgain[...].reshape(1, ds), (LANES, ds)))

    def weigh(k, carry):
        cols = pl.ds(pl.multiple_of(k * LANES, LANES), LANES)
        scaled = (sp[:, cols].astype(F32) * gain_col).astype(BF16)
        sw[:, cols] = scaled
        wt_out[cols, :] = jnp.transpose(scaled)
        return carry

    lax.fori_loop(0, embed // LANES, weigh, 0)
    pooling(3)

    others[1].wait()
    partial = jnp.dot(tpool[...].astype(BF16), tp[...], preferred_element_type=F32)
    for j in range(n):
        block = partial[j * rows : (j + 1) * rows]
        pf[j] = block
        pb[j] = block.astype(BF16)
    rs_copies = []
    for o in range(1, n):
        copy = remote(pb.at[lax.rem(me_m + o, n)], pr.at[o], rs_send.at[o], rs_recv.at[o], mp_peer(o))
        copy.start()
        rs_copies.append(copy)

    others[2].wait()
    tiles = embed // TILE
    stages = (ua, ub)

    def chunk(c):
        return pl.ds(pl.multiple_of(c * tokens, tokens), tokens)

    def multiply(c, k, out):
        out[...] = jnp.dot(x_out[chunk(c), :], sw[:, k * TILE : (k + 1) * TILE], preferred_element_type=F32)

    def rescale(c):
        x = x_out[chunk(c), :].astype(F32)
        scale = lax.rsqrt(jnp.mean(x * x, axis=-1, keepdims=True) + 1e-06)
        scl_out[chunk(c), :] = live_col[chunk(c), :] * scale

    group8 = lax.broadcasted_iota(jnp.int32, (2 * per_tile, tokens), 0)
    token8 = lax.broadcasted_iota(jnp.int32, (2 * per_tile, tokens), 1) // qlen
    picks = [jnp.where(group8 == token8 + s * per_tile, 1.0, 0.0).astype(BF16) for s in range(2)]

    def activate(c, i, side, k, held):
        cols = slice(k * TILE, (k + 1) * TILE)
        scale = scl_out[chunk(c), :]
        u = held[...] * jnp.concatenate([scale] * (TILE // LANES), axis=1)
        z = (u * (ROOT + (ROOT * CUBE) * (u * u))).astype(BF16)
        ul = u.astype(BF16)
        th = jnp.tanh(z)
        part = th * BF16(0.5) + BF16(0.5)
        act = ul * part
        bend = (ul * ul) * BF16(3.0 * ROOT * CUBE) + BF16(ROOT)
        h_out[chunk(c), cols] = part + act * (BF16(1.0) - th) * bend
        summed = jnp.dot(picks[side], act, preferred_element_type=F32)
        spot = pl.ds(pl.multiple_of(i * 2 * per_tile, 2 * per_tile), 2 * per_tile)
        if side == 0:
            raw_out[spot, cols] = summed
        else:
            raw_out[spot, cols] += summed

    def student(i, carry):
        here = (2 * i, 2 * i + 1)
        after = jnp.minimum(2 * i + 2, 2 * bodies - 1)
        for side in range(2):
            for k in range(tiles):
                step = side * tiles + k
                if k + 1 < tiles:
                    multiply(here[side], k + 1, stages[(step + 1) % 2])
                else:
                    multiply(here[1] if side == 0 else after, 0, stages[(step + 1) % 2])
                if k == 0:
                    rescale(here[1] if side == 0 else after)
                activate(here[side], i, side, k, stages[step % 2])
        return carry

    rescale(0)
    multiply(0, 0, stages[0])
    first, second, third = bodies // 2, 3 * bodies // 4, bodies
    lax.fori_loop(0, first, student, 0)

    for copy in rs_copies:
        copy.wait_recv()
    summed = pf[me_m]
    for o in range(1, n):
        summed = summed + pr[o].astype(F32)
    unit = summed * lax.rsqrt(jnp.mean(summed * summed, axis=-1, keepdims=True) + 1e-06) * (embed ** -0.5)
    te[me_d, core, chip] = unit.astype(BF16)
    order = nearest(dn)
    dp_copies, col_copies, fw_copies = {}, {}, {}
    for o in order:
        own = te.at[me_d, core, chip]
        dp_copies[o] = remote(own, own, dp_send.at[o], dp_recv.at[o], dp_peer(o))
        dp_copies[o].start()

    def share(o):
        block = te.at[lax.rem(me_d + dn - o, dn), core, chip]
        for p in range(1, half):
            col_copies[o, p] = remote(block, block, col_send.at[o, p], col_recv.at[o, p], col_peer(p))
            col_copies[o, p].start()

    def pass_on(o):
        for p in range(1, half):
            col_copies[o, p].wait_recv()
        block = te.at[lax.rem(me_d + dn - o, dn), core]
        fw_copies[o] = remote(block, block, fw_send.at[o], fw_recv.at[o], partner)
        fw_copies[o].start()

    share(0)
    lax.fori_loop(first, second, student, 0)
    for o in order[: len(order) // 2]:
        dp_copies[o].wait_recv()
        share(o)
    pass_on(0)
    lax.fori_loop(second, third, student, 0)
    for o in order[len(order) // 2 :]:
        dp_copies[o].wait_recv()
        share(o)

    raw = raw_out[...]
    scale = lax.rsqrt(jnp.mean(raw * raw, axis=-1, keepdims=True) + 1e-06)
    unit = scale * (embed ** -0.5)
    sround = (raw * unit).astype(BF16)
    total = dn * passages
    place = lax.broadcasted_iota(jnp.int32, (total, queries), 0)
    block, row = place // rows, lax.rem(place, rows)
    owner, slot = block // n, lax.rem(block, n)
    lines = (owner * n + lax.rem(slot, half) * 2 + slot // half) * rows + row
    picker = jnp.transpose(jnp.where(pos[...].reshape(1, queries) == lines, 1.0, 0.0)).astype(BF16)

    for o in order:
        pass_on(o)
    for o in [0] + order:
        fw_copies[o].wait_recv()
    table = te[...].reshape(total, embed)
    tpos = jnp.dot(picker, table, preferred_element_type=F32).astype(BF16)
    both = jnp.concatenate([tpos, sround], axis=0)
    logits = lax.dot_general(both, table, NT, preferred_element_type=F32)
    texp = jnp.exp(10.0 * logits[:queries])
    sexp = jnp.exp(20.0 * logits[queries:])
    diff = sexp / jnp.sum(sexp, axis=1, keepdims=True) - texp / jnp.sum(texp, axis=1, keepdims=True)
    ge = 20.0 * jnp.dot(diff.astype(BF16), table, preferred_element_type=F32)
    ge_out[...] = ge
    inner = jnp.mean(raw * ge, axis=-1, keepdims=True)
    grad_out[...] = unit * (ge - raw * (scale * scale * inner))
    for copy in sq_copies + rs_copies + list(dp_copies.values()) + list(col_copies.values()) + list(fw_copies.values()):
        copy.wait_send()


def back(ge, grad, h, xs, scl, wt, embed_out, states_out, ga, gb, staged, embed_sem, sem):
    total, embed = h.shape
    ds = xs.shape[1]
    queries = grad.shape[0]
    qlen = total // queries
    tokens = TILE
    count = total // tokens
    per_tile = tokens // qlen
    keep = pltpu.make_async_copy(ge, embed_out, embed_sem)
    keep.start()

    def chunk(c):
        return pl.ds(pl.multiple_of(c * tokens, tokens), tokens)

    def store(c):
        return pltpu.make_async_copy(staged.at[chunk(c)], states_out.at[chunk(c)], sem.at[c])

    def multiply(c, out):
        pieces = []
        for j in range(per_tile):
            line = jnp.broadcast_to(grad[pl.ds(c * per_tile + j, 1), :], (16, embed)).astype(BF16)
            part = pl.ds(pl.multiple_of(c * tokens + j * qlen, qlen), qlen)
            pieces.append(h[part, :] * jnp.concatenate([line] * (qlen // 16), axis=0))
        out[...] = jnp.dot(jnp.concatenate(pieces, axis=0), wt[...], preferred_element_type=F32)

    def finish(c, held):
        gy = held[...]
        x = xs[chunk(c), :].astype(F32)
        scale = scl[chunk(c), :]
        inner = jnp.mean(x * gy, axis=-1, keepdims=True)
        bias = scale * scale * inner
        wide = lambda v: jnp.concatenate([v] * (ds // LANES), axis=1)
        staged[chunk(c), :] = (wide(scale) * (gy - x * wide(bias))).astype(BF16)
        store(c).start()

    multiply(0, ga)

    def body(i, carry):
        multiply(2 * i + 1, gb)
        finish(2 * i, ga)
        multiply(2 * i + 2, ga)
        finish(2 * i + 1, gb)
        return carry

    lax.fori_loop(0, count // 2 - 1, body, 0)
    multiply(count - 1, gb)
    finish(count - 2, ga)
    finish(count - 1, gb)
    keep.wait()
    for c in range(count):
        store(c).wait()


def shards(dn, n, ts, tgain, tproj, tmask, ss, sgain, sproj, smask, positive):
    passages, length, feats = ts.shape
    embed = tproj.shape[1]
    queries, qlen, ds = ss.shape
    rows = passages // n
    total = queries * qlen
    chunks = passages // 8
    flat = ss.reshape(total, ds)
    hbm = pl.BlockSpec(memory_space=pltpu.HBM)
    vmem = pl.BlockSpec(memory_space=pltpu.VMEM)
    dma = pltpu.SemaphoreType.DMA
    ge, grad, h, xs, scl, wt = pl.pallas_call(
        functools.partial(front, dn, n),
        out_shape=(
            pltpu.VMEM((queries, embed), F32),
            pltpu.VMEM((queries, embed), F32),
            pltpu.VMEM((total, embed), BF16),
            pltpu.VMEM((total, ds), BF16),
            pltpu.VMEM((total, LANES), F32),
            pltpu.VMEM((embed, ds), BF16),
        ),
        in_specs=[hbm, vmem, vmem, hbm, hbm, vmem, hbm, vmem, vmem],
        out_specs=(vmem,) * 6,
        scratch_shapes=[
            pltpu.VMEM((passages, length, feats), BF16),
            pltpu.VMEM((feats, embed), BF16),
            pltpu.VMEM((ds, embed), BF16),
            pltpu.VMEM((ds, embed), BF16),
            pltpu.VMEM((total, LANES), F32),
            pltpu.VMEM((chunks, 8, length), F32),
            pltpu.VMEM((n, chunks, 8, length), F32),
            pltpu.VMEM((passages, feats), F32),
            pltpu.VMEM((n, rows, embed), F32),
            pltpu.VMEM((n, rows, embed), BF16),
            pltpu.VMEM((n, rows, embed), BF16),
            pltpu.VMEM((dn, 2, n // 2, rows, embed), BF16),
            pltpu.VMEM((queries, embed), F32),
            pltpu.VMEM((TILE, TILE), F32),
            pltpu.VMEM((TILE, TILE), F32),
            dma((chunks,)),
            dma((3,)),
            dma((n, GROUPS)),
            dma((n, GROUPS)),
            dma((n,)),
            dma((n,)),
            dma((dn,)),
            dma((dn,)),
            dma((dn, n // 2)),
            dma((dn, n // 2)),
            dma((dn,)),
            dma((dn,)),
        ],
        compiler_params=pltpu.CompilerParams(
            collective_id=0, has_side_effects=True, vmem_limit_bytes=56_600_000
        ),
        name="front",
    )(ts, tmask, tgain, tproj, flat, sgain, sproj, smask, positive)
    grad_embed, grad_states = pl.pallas_call(
        back,
        out_shape=(jax.ShapeDtypeStruct((queries, embed), F32), jax.ShapeDtypeStruct((total, ds), BF16)),
        in_specs=[vmem] * 6,
        out_specs=(hbm, hbm),
        scratch_shapes=[
            pltpu.VMEM((TILE, ds), F32),
            pltpu.VMEM((TILE, ds), F32),
            pltpu.VMEM((total, ds), BF16),
            dma,
            dma((total // TILE,)),
        ],
        compiler_params=pltpu.CompilerParams(vmem_limit_bytes=16 * 1024 * 1024),
        name="back",
    )(ge, grad, h, xs, scl, wt)
    return grad_embed, grad_states.reshape(queries, qlen, ds)


def solution(mesh):
    in_specs = (
        P("dp", None, "mp"),
        P("mp"),
        P("mp", None),
        P("dp", None),
        P(("dp", "mp"), None, None),
        P(),
        P(),
        P(("dp", "mp"), None),
        P(("dp", "mp")),
    )
    out_specs = (P(("dp", "mp"), None), P(("dp", "mp"), None, None))
    body = functools.partial(shards, mesh.shape["dp"], mesh.shape["mp"])
    return jax.shard_map(body, mesh=mesh, in_specs=in_specs, out_specs=out_specs, check_vma=False)
```

```python
import functools

import jax
import jax.numpy as jnp
from jax import lax
from jax.experimental import pallas as pl
from jax.experimental.pallas import tpu as pltpu
from jax.sharding import PartitionSpec as P

MESH = pl.DeviceIdType.MESH
F32 = jnp.float32
BF16 = jnp.bfloat16
GROUPS = 4
AHEAD = 5
ROOT = 0.7978845608028654
CUBE = 0.044715
LANES = 128
TILE = 256
SLAB = 16
NT = (((1,), (1,)), ((), ()))


def nearest(count):
    return [sorted(range(count), key=lambda other: abs(other - here))[1:] for here in range(count)]


def choose(index, values):
    picked = values[0]
    for i, value in enumerate(values[1:], 1):
        picked = jnp.where(index == i, value, picked)
    return picked


def front(
    dn, n, ts, tmask, tgain, tproj, ss, sgain, sproj, smask, pos,
    ge_out, grad_out, h_out, x_out, scl_out, wt_out,
    tx, tp, sp, sw, tm, tg, sg, sm, po, live_col, sq, sqr, tpool, pf, pb, pr, te, raw_out, ua, ub, aa, ab, ca, cb,
    sem_tx, sem_in, sq_send, sq_recv, rs_send, rs_recv, z_send, z_recv, plane_send, plane_recv, fw_send, fw_recv,
):
    passages, length, feats = tx.shape
    width = n * feats
    rows = passages // n
    embed = tp.shape[1]
    chunks = passages // 8
    queries, qlen = sm.shape
    ds = sp.shape[0]
    tokens = TILE
    per_tile = tokens // qlen
    me_d, me_m = lax.axis_index("dp"), lax.axis_index("mp")
    half = n // 2
    core, chip = lax.rem(me_m, 2), me_m // 2

    def mp_peer(o):
        return (me_d, lax.rem(me_m + o, n))

    def dp_peer(o):
        return (lax.rem(me_d + o, dn), me_m)

    side_x = 2 if dn % 2 == 0 else 1
    depth = dn // side_x
    me_z, me_x = me_d // side_x, lax.rem(me_d, side_x)

    def plane_peer(p):
        x = lax.rem(me_x + p // half, side_x)
        return (me_z * side_x + x, 2 * lax.rem(chip + p % half, half) + core)

    partner = (me_d, me_m + 1 - 2 * core)

    def load(c):
        part = pl.ds(c * 8, 8)
        return pltpu.make_async_copy(ts.at[part], tx.at[part], sem_tx.at[lax.rem(c, ahead)])

    ahead = min(AHEAD, chunks)
    moves = [(smask, sm), (tmask, tm), (tgain, tg), (sgain, sg), (pos, po), (tproj, tp), (sproj, sp), (ss, x_out)]
    copies = [pltpu.make_async_copy(a, b, sem_in.at[i]) for i, (a, b) in enumerate(moves)]
    small, others = copies[:5], copies[5:]
    for copy in small:
        copy.start()
    for c in range(ahead):
        load(c).start()
    barrier = pltpu.get_barrier_semaphore()
    for o in range(1, n):
        pl.semaphore_signal(barrier, inc=1, device_id=mp_peer(o), device_id_type=MESH)
    for o in range(1, dn):
        pl.semaphore_signal(barrier, inc=1, device_id=dp_peer(o), device_id_type=MESH)

    def remote(src, dst, send, recv, peer):
        return pltpu.make_async_remote_copy(
            src_ref=src, dst_ref=dst, send_sem=send, recv_sem=recv, device_id=peer, device_id_type=MESH
        )

    def spread_mask():
        for copy in small:
            copy.wait()
        turned = jnp.transpose(sm[...].astype(F32))
        for q in range(queries):
            live_col[q * qlen : (q + 1) * qlen, :] = jnp.broadcast_to(turned[:, q : q + 1], (qlen, LANES))

    ones = jnp.ones((16, TILE), BF16)
    row8 = lax.broadcasted_iota(jnp.int32, (8, length), 0)
    row16 = lax.rem(lax.broadcasted_iota(jnp.int32, (16, length), 0), 8)
    per = chunks // GROUPS

    def squares(c, carry):
        load(c).wait()

        @pl.when(c + ahead < chunks)
        def _():
            load(c + ahead).start()

        held = jnp.zeros((8, length), F32)
        for j in range(8):
            terms = []
            for k in range(feats // TILE):
                x = tx[c * 8 + j, :, k * TILE : (k + 1) * TILE]
                terms.append(x * x)
            while len(terms) > 1:
                terms = [a + b for a, b in zip(terms[::2], terms[1::2])] + terms[len(terms) // 2 * 2 :]
            line = lax.dot_general(ones, terms[0], NT, preferred_element_type=F32)
            held = jnp.where(row8 == j, line[:8], held)
        sq[c] = held
        return carry

    def send_squares(g):
        part = pl.ds(g * per, per)
        for o in range(1, n):
            remote(sq.at[part], sqr.at[g, o - 1], sq_send, sq_recv.at[g], mp_peer(o)).start()

    def pool(g, i, carry):
        c = g * per + i
        total = sq[c]
        for o in range(1, n):
            total = total + sqr[g, o - 1, i]
        part = pl.ds(pl.multiple_of(c * 8, 8), 8)
        weight = tm[part, :].astype(F32) * lax.rsqrt(total / width + 1e-06)
        high = weight.astype(BF16).astype(F32)
        both = jnp.concatenate([high, weight - high], axis=0)
        left = jnp.concatenate([jnp.where(row16 == j, both, 0.0) for j in range(8)], axis=1).astype(BF16)
        sums = jnp.dot(left, tx[pl.ds(c * 8, 8)].reshape(8 * length, feats), preferred_element_type=F32)
        tpool[part, :] = (sums[:8] + sums[8:]) * tg[...].reshape(1, feats)
        return carry

    def pooling(g):
        remote(sqr.at[g], sqr.at[g], sq_send, sq_recv.at[g], partner).wait_recv()
        lax.fori_loop(0, per, functools.partial(pool, g), 0)

    lax.fori_loop(0, per, squares, 0)
    pl.semaphore_wait(barrier, n + dn - 2)
    send_squares(0)
    lax.fori_loop(per, 2 * per, squares, 0)
    for copy in others:
        copy.start()
    send_squares(1)
    spread_mask()
    lax.fori_loop(2 * per, 3 * per, squares, 0)
    send_squares(2)
    lax.fori_loop(3 * per, 4 * per, squares, 0)
    send_squares(3)
    for g in range(GROUPS):
        pooling(g)

    others[0].wait()
    partial = jnp.dot(tpool[...].astype(BF16), tp[...], preferred_element_type=F32)
    for j in range(n):
        block = partial[j * rows : (j + 1) * rows]
        pf[j] = block
        pb[j] = block.astype(BF16)
    for o in range(1, n):
        remote(pb.at[lax.rem(me_m + o, n)], pr.at[o - 1], rs_send, rs_recv, mp_peer(o)).start()

    others[1].wait()
    gain_col = jnp.transpose(jnp.broadcast_to(sg[...].reshape(1, ds), (LANES, ds)))

    def weigh(k, carry):
        cols = pl.ds(pl.multiple_of(k * LANES, LANES), LANES)
        scaled = (sp[:, cols].astype(F32) * gain_col).astype(BF16)
        sw[k] = scaled
        for j in range(ds // LANES):
            wt_out[j, cols, :] = jnp.transpose(scaled[j * LANES : (j + 1) * LANES])
        return carry

    lax.fori_loop(0, embed // LANES, weigh, 0)
    others[2].wait()
    stages = ((ua, aa, ca), (ub, ab, cb))
    count = queries // per_tile

    def chunk(c):
        return pl.ds(pl.multiple_of(c * tokens, tokens), tokens)

    tiles = embed // TILE

    def prepare(c, side, k):
        out, _, scale_out = stages[side]
        right = jnp.concatenate([sw[k * (TILE // LANES) + j] for j in range(TILE // LANES)], axis=1)
        out[:, k * TILE : (k + 1) * TILE] = jnp.dot(x_out[chunk(c), :], right, preferred_element_type=F32)

    def rescale(c, side, k):
        scale_out = stages[side][2]
        for r in range(k * tokens // tiles, (k + 1) * tokens // tiles, SLAB):
            part = pl.ds(pl.multiple_of(c * tokens + r, SLAB), SLAB)
            x = x_out[part, :].astype(F32)
            scale = live_col[part, :] * lax.rsqrt(jnp.mean(x * x, axis=-1, keepdims=True) + 1e-06)
            scale_out[r : r + SLAB, :] = scale
            scl_out[part, :] = scale

    group8 = lax.broadcasted_iota(jnp.int32, (2 * per_tile, tokens), 0)
    token8 = lax.broadcasted_iota(jnp.int32, (2 * per_tile, tokens), 1) // qlen
    picks = [jnp.where(group8 == token8 + side * per_tile, 1.0, 0.0).astype(BF16) for side in range(2)]

    def activate(c, side, k):
        held, kept, scale_in = stages[side]
        cols = slice(k * TILE, (k + 1) * TILE)
        for r in range(0, tokens, SLAB):
            u = held[r : r + SLAB, cols] * jnp.concatenate([scale_in[r : r + SLAB, :]] * (TILE // LANES), axis=1)
            z = (u * (ROOT + (ROOT * CUBE) * (u * u))).astype(BF16)
            ul = u.astype(BF16)
            th = jnp.tanh(z)
            part = th * BF16(0.5) + BF16(0.5)
            act = ul * part
            bend = (ul * ul) * BF16(3.0 * ROOT * CUBE) + BF16(ROOT)
            kept[r : r + SLAB, cols] = act
            spot = pl.ds(pl.multiple_of(c * tokens + r, SLAB), SLAB)
            h_out[spot, cols] = part + act * (BF16(1.0) - th) * bend

    def total_up(c, side, k):
        cols = slice(k * TILE, (k + 1) * TILE)
        summed = jnp.dot(picks[side], stages[side][1][:, cols], preferred_element_type=F32)
        spot = pl.ds(pl.multiple_of(c // 2 * (2 * per_tile), 2 * per_tile), 2 * per_tile)
        if side == 0:
            raw_out[spot, cols] = summed
        else:
            raw_out[spot, cols] += summed

    def student(c, carry):
        for side in range(2):

            @pl.when(lax.rem(c, 2) == side)
            def _():
                for k in range(tiles):
                    total_up(jnp.maximum(c - 1, 0), 1 - side, k)
                    rescale(jnp.minimum(c + 1, count - 1), 1 - side, k)
                for k in range(tiles):
                    prepare(jnp.minimum(c + 1, count - 1), 1 - side, k)
                    activate(c, side, k)

        return carry

    ab[...] = jnp.zeros_like(ab)
    raw_out[...] = jnp.zeros_like(raw_out)
    for k in range(tiles):
        prepare(0, 0, k)
        rescale(0, 0, k)
    marks = [count * j // 8 for j in (0, 2, 4, 5, 6, 7, 8)]

    def work(stage):
        lax.fori_loop(marks[stage], marks[stage + 1], student, 0)

    work(0)
    remote(pr, pr, rs_send, rs_recv, partner).wait_recv()
    summed = pf[me_m]
    for o in range(1, n):
        summed = summed + pr[o - 1].astype(F32)
    unit = summed * lax.rsqrt(jnp.mean(summed * summed, axis=-1, keepdims=True) + 1e-06) * (embed ** -0.5)
    te[me_z, core, me_x, chip] = unit.astype(BF16)
    order = nearest(depth)
    peers = side_x * half - 1
    own = te.at[me_z, core, me_x, chip]
    gathered = te.reshape(depth * 2 * side_x * half, rows, embed).at[pl.ds(0, peers)]

    def near(j):
        return choose(me_z, [order[z][j] for z in range(depth)])

    for j in range(depth - 1):
        z = near(depth - 2 - j)
        remote(own, own, z_send, z_recv.at[me_z], (z * side_x + me_x, me_m)).start()

    def share(z):
        block = te.at[z, core, me_x, chip]
        for p in range(peers, 0, -1):
            remote(block, block, plane_send, plane_recv.at[z], plane_peer(p)).start()

    def pass_on(z):
        if peers:
            remote(gathered, gathered, plane_send, plane_recv.at[z], partner).wait_recv()
        block = te.at[z, core]
        remote(block, block, fw_send, fw_recv.at[z], partner).start()

    def relay(j):
        z = near(j)
        block = te.at[z, core, me_x, chip]
        remote(block, block, z_send, z_recv.at[z], partner).wait_recv()
        share(z)

    share(me_z)
    work(1)
    for j in range(depth - 1):
        relay(j)
        if j < 3:
            work(2 + j)
        if j == 1:
            pass_on(me_z)
    for j in range(min(3, depth - 1), 4):
        work(2 + j)
    for k in range(tiles):
        total_up(count - 1, 1, k)
    for j in range(depth - 2):
        pass_on(near(j))

    raw = raw_out[...]
    scale = lax.rsqrt(jnp.mean(raw * raw, axis=-1, keepdims=True) + 1e-06)
    unit = scale * (embed ** -0.5)
    sround = (raw * unit).astype(BF16)
    total = dn * passages
    place = lax.broadcasted_iota(jnp.int32, (total, queries), 0)
    block, row = place // rows, lax.rem(place, rows)
    plane, slot = block // (side_x * n), lax.rem(block, side_x * n)
    owner = plane * side_x + lax.rem(slot // half, side_x)
    member = lax.rem(slot, half) * 2 + slot // (half * side_x)
    lines = (owner * n + member) * rows + row
    picker = jnp.transpose(jnp.where(po[...].reshape(1, queries) == lines, 1.0, 0.0)).astype(BF16)

    pass_on(near(depth - 2))
    for j in range(depth):
        span = te.at[me_z, core]
        remote(span, span, fw_send, fw_recv.at[j], partner).wait_recv()
    table = te[...].reshape(total, embed)
    tpos = jnp.dot(picker, table, preferred_element_type=F32).astype(BF16)
    both = jnp.concatenate([tpos, sround], axis=0)
    logits = lax.dot_general(both, table, NT, preferred_element_type=F32)
    texp = jnp.exp(10.0 * logits[:queries])
    sexp = jnp.exp(20.0 * logits[queries:])
    diff = sexp / jnp.sum(sexp, axis=1, keepdims=True) - texp / jnp.sum(texp, axis=1, keepdims=True)
    ge = 20.0 * jnp.dot(diff.astype(BF16), table, preferred_element_type=F32)
    ge_out[...] = ge
    inner = jnp.mean(raw * ge, axis=-1, keepdims=True)
    grad_out[...] = unit * (ge - raw * (scale * scale * inner))
    remote(sqr, sqr, sq_send, sq_recv.at[0], partner).wait_send()
    remote(pr, pr, rs_send, rs_recv, partner).wait_send()
    sent = te.at[pl.ds(0, depth - 1), 0, 0, 0]
    remote(sent, sent, z_send, z_recv.at[0], partner).wait_send()
    if peers:
        for z in range(depth):
            remote(gathered, gathered, plane_send, plane_recv.at[0], partner).wait_send()
    sent = te.at[:, 0]
    remote(sent, sent, fw_send, fw_recv.at[0], partner).wait_send()


def back(ge, grad, h, xs, scl, wt, embed_out, states_out, ga, gb, staged, embed_sem, sem):
    total, embed = h.shape
    ds = xs.shape[1]
    queries = grad.shape[0]
    qlen = total // queries
    tokens = TILE
    count = total // tokens
    per_tile = tokens // qlen
    keep = pltpu.make_async_copy(ge, embed_out, embed_sem)
    keep.start()

    def chunk(c):
        return pl.ds(pl.multiple_of(c * tokens, tokens), tokens)

    def store(c):
        return pltpu.make_async_copy(staged.at[chunk(c)], states_out.at[chunk(c)], sem.at[c])

    def multiply(c, out):
        pieces = []
        for j in range(per_tile):
            line = jnp.broadcast_to(grad[pl.ds(c * per_tile + j, 1), :], (16, embed)).astype(BF16)
            part = pl.ds(pl.multiple_of(c * tokens + j * qlen, qlen), qlen)
            pieces.append(h[part, :] * jnp.concatenate([line] * (qlen // 16), axis=0))
        left = jnp.concatenate(pieces, axis=0)
        for k in range(ds // TILE):
            right = jnp.concatenate([wt[k * (TILE // LANES) + j] for j in range(TILE // LANES)], axis=1)
            out[:, k * TILE : (k + 1) * TILE] = jnp.dot(left, right, preferred_element_type=F32)

    def finish(c, held):
        gy = held[...]
        x = xs[chunk(c), :].astype(F32)
        scale = scl[chunk(c), :]
        inner = jnp.mean(x * gy, axis=-1, keepdims=True)
        bias = scale * scale * inner
        wide = lambda v: jnp.concatenate([v] * (ds // LANES), axis=1)
        staged[chunk(c), :] = (wide(scale) * (gy - x * wide(bias))).astype(BF16)
        store(c).start()

    multiply(0, ga)

    def body(i, carry):
        multiply(2 * i + 1, gb)
        finish(2 * i, ga)
        multiply(2 * i + 2, ga)
        finish(2 * i + 1, gb)
        return carry

    lax.fori_loop(0, count // 2 - 1, body, 0)
    multiply(count - 1, gb)
    finish(count - 2, ga)
    finish(count - 1, gb)
    keep.wait()
    for c in range(count):
        store(c).wait()


def shards(dn, n, ts, tgain, tproj, tmask, ss, sgain, sproj, smask, positive):
    passages, length, feats = ts.shape
    embed = tproj.shape[1]
    queries, qlen, ds = ss.shape
    rows = passages // n
    total = queries * qlen
    chunks = passages // 8
    side_x = 2 if dn % 2 == 0 else 1
    flat = ss.reshape(total, ds)
    hbm = pl.BlockSpec(memory_space=pltpu.HBM)
    vmem = pl.BlockSpec(memory_space=pltpu.VMEM)
    dma = pltpu.SemaphoreType.DMA
    ge, grad, h, xs, scl, wt = pl.pallas_call(
        functools.partial(front, dn, n),
        out_shape=(
            pltpu.VMEM((queries, embed), F32),
            pltpu.VMEM((queries, embed), F32),
            pltpu.VMEM((total, embed), BF16),
            pltpu.VMEM((total, ds), BF16),
            pltpu.VMEM((total, LANES), F32),
            pltpu.VMEM((ds // LANES, embed, LANES), BF16),
        ),
        in_specs=[hbm] * 9,
        out_specs=(vmem,) * 6,
        scratch_shapes=[
            pltpu.VMEM((passages, length, feats), BF16),
            pltpu.VMEM((feats, embed), BF16),
            pltpu.VMEM((ds, embed), BF16),
            pltpu.VMEM((embed // LANES, ds, LANES), BF16),
            pltpu.VMEM((passages, length), jnp.int32),
            pltpu.VMEM((feats,), F32),
            pltpu.VMEM((ds,), F32),
            pltpu.VMEM((queries, qlen), jnp.int32),
            pltpu.VMEM((queries,), jnp.int32),
            pltpu.VMEM((total, LANES), F32),
            pltpu.VMEM((chunks, 8, length), F32),
            pltpu.VMEM((GROUPS, n - 1, chunks // GROUPS, 8, length), F32),
            pltpu.VMEM((passages, feats), F32),
            pltpu.VMEM((n, rows, embed), F32),
            pltpu.VMEM((n, rows, embed), BF16),
            pltpu.VMEM((n - 1, rows, embed), BF16),
            pltpu.VMEM((dn // side_x, 2, side_x, n // 2, rows, embed), BF16),
            pltpu.VMEM((queries, embed), F32),
            pltpu.VMEM((TILE, embed), F32),
            pltpu.VMEM((TILE, embed), F32),
            pltpu.VMEM((TILE, embed), BF16),
            pltpu.VMEM((TILE, embed), BF16),
            pltpu.VMEM((TILE, LANES), F32),
            pltpu.VMEM((TILE, LANES), F32),
            dma((min(AHEAD, chunks),)),
            dma((8,)),
            dma,
            dma((GROUPS,)),
            dma,
            dma,
            dma,
            dma((dn // side_x,)),
            dma,
            dma((dn // side_x,)),
            dma,
            dma((dn // side_x,)),
        ],
        compiler_params=pltpu.CompilerParams(
            collective_id=0, has_side_effects=True, vmem_limit_bytes=56_600_000
        ),
        name="front",
    )(ts, tmask, tgain, tproj, flat, sgain, sproj, smask, positive)
    grad_embed, grad_states = pl.pallas_call(
        back,
        out_shape=(jax.ShapeDtypeStruct((queries, embed), F32), jax.ShapeDtypeStruct((total, ds), BF16)),
        in_specs=[vmem] * 6,
        out_specs=(hbm, hbm),
        scratch_shapes=[
            pltpu.VMEM((TILE, ds), F32),
            pltpu.VMEM((TILE, ds), F32),
            pltpu.VMEM((total, ds), BF16),
            dma,
            dma((total // TILE,)),
        ],
        compiler_params=pltpu.CompilerParams(vmem_limit_bytes=16 * 1024 * 1024),
        name="back",
    )(ge, grad, h, xs, scl, wt)
    return grad_embed, grad_states.reshape(queries, qlen, ds)


def solution(mesh):
    in_specs = (
        P("dp", None, "mp"),
        P("mp"),
        P("mp", None),
        P("dp", None),
        P(("dp", "mp"), None, None),
        P(),
        P(),
        P(("dp", "mp"), None),
        P(("dp", "mp")),
    )
    out_specs = (P(("dp", "mp"), None), P(("dp", "mp"), None, None))
    body = functools.partial(shards, mesh.shape["dp"], mesh.shape["mp"])
    return jax.shard_map(body, mesh=mesh, in_specs=in_specs, out_specs=out_specs, check_vma=False)
```

```python
import functools

import jax
import jax.numpy as jnp
from jax import lax
from jax.experimental import pallas as pl
from jax.experimental.pallas import tpu as pltpu
from jax.sharding import PartitionSpec as P

MESH = pl.DeviceIdType.MESH
F32 = jnp.float32
BF16 = jnp.bfloat16
GROUPS = 4
AHEAD = 5
ROOT = 0.7978845608028654
CUBE = 0.044715
LANES = 128
TILE = 256
SLAB = 16
NT = (((1,), (1,)), ((), ()))


def nearest(count):
    return [sorted(range(count), key=lambda other: abs(other - here))[1:] for here in range(count)]


def halves_of(passages, n):
    return 2 if passages // n % 16 == 0 else 1


def choose(index, values):
    picked = values[0]
    for i, value in enumerate(values[1:], 1):
        picked = jnp.where(index == i, value, picked)
    return picked


def front(
    dn, n, ts, tmask, tgain, tproj, ss, sgain, sproj, smask, pos,
    ge_out, grad_out, h_out, x_out, scl_out, wt_out,
    tx, tp, sp, sw, tm, tg, sg, sm, po, live_col, sq, sqr, tpool, pf, pb, pr, te, raw_out, ua, ub, aa, ab, ca, cb,
    sem_tx, sem_in, sq_send, sq_recv, rs_send, rs_recv, z_send, z_recv, plane_send, plane_recv, fw_send, fw_recv,
):
    passages, length, feats = tx.shape
    width = n * feats
    parts = halves_of(passages, n)
    rows = passages // (n * parts)
    span = passages // parts
    embed = tp.shape[1]
    chunks = passages // 8
    queries, qlen = sm.shape
    ds = sp.shape[0]
    tokens = TILE
    per_tile = tokens // qlen
    me_d, me_m = lax.axis_index("dp"), lax.axis_index("mp")
    half = n // 2
    core, chip = lax.rem(me_m, 2), me_m // 2

    def mp_peer(o):
        return (me_d, lax.rem(me_m + o, n))

    def dp_peer(o):
        return (lax.rem(me_d + o, dn), me_m)

    side_x = 2 if dn % 2 == 0 else 1
    depth = dn // side_x
    me_z, me_x = me_d // side_x, lax.rem(me_d, side_x)

    def plane_peer(p):
        x = lax.rem(me_x + p // half, side_x)
        return (me_z * side_x + x, 2 * lax.rem(chip + p % half, half) + core)

    partner = (me_d, me_m + 1 - 2 * core)

    def load(c):
        part = pl.ds(c * 8, 8)
        return pltpu.make_async_copy(ts.at[part], tx.at[part], sem_tx.at[lax.rem(c, ahead)])

    ahead = min(AHEAD, chunks)
    moves = [(smask, sm), (tmask, tm), (tgain, tg), (sgain, sg), (pos, po), (tproj, tp), (sproj, sp), (ss, x_out)]
    copies = [pltpu.make_async_copy(a, b, sem_in.at[i]) for i, (a, b) in enumerate(moves)]
    small, others = copies[:5], copies[5:]
    for copy in small:
        copy.start()
    for c in range(ahead):
        load(c).start()
    barrier = pltpu.get_barrier_semaphore()
    for o in range(1, n):
        pl.semaphore_signal(barrier, inc=1, device_id=mp_peer(o), device_id_type=MESH)
    for o in range(1, dn):
        pl.semaphore_signal(barrier, inc=1, device_id=dp_peer(o), device_id_type=MESH)

    def remote(src, dst, send, recv, peer):
        return pltpu.make_async_remote_copy(
            src_ref=src, dst_ref=dst, send_sem=send, recv_sem=recv, device_id=peer, device_id_type=MESH
        )

    def spread_mask():
        for copy in small:
            copy.wait()
        turned = jnp.transpose(sm[...].astype(F32))
        for q in range(queries):
            live_col[q * qlen : (q + 1) * qlen, :] = jnp.broadcast_to(turned[:, q : q + 1], (qlen, LANES))

    ones = jnp.ones((16, TILE), BF16)
    row8 = lax.broadcasted_iota(jnp.int32, (8, length), 0)
    row16 = lax.rem(lax.broadcasted_iota(jnp.int32, (16, length), 0), 8)
    per = chunks // GROUPS

    def squares(c, carry):
        load(c).wait()

        @pl.when(c + ahead < chunks)
        def _():
            load(c + ahead).start()

        held = jnp.zeros((8, length), F32)
        for j in range(8):
            terms = []
            for k in range(feats // TILE):
                x = tx[c * 8 + j, :, k * TILE : (k + 1) * TILE]
                terms.append(x * x)
            while len(terms) > 1:
                terms = [a + b for a, b in zip(terms[::2], terms[1::2])] + terms[len(terms) // 2 * 2 :]
            line = lax.dot_general(ones, terms[0], NT, preferred_element_type=F32)
            held = jnp.where(row8 == j, line[:8], held)
        sq[c] = held
        return carry

    def send_squares(g):
        part = pl.ds(g * per, per)
        for o in range(1, n):
            remote(sq.at[part], sqr.at[g, o - 1], sq_send, sq_recv.at[g], mp_peer(o)).start()

    def pool(g, i, carry):
        c = g * per + i
        total = sq[c]
        for o in range(1, n):
            total = total + sqr[g, o - 1, i]
        part = pl.ds(pl.multiple_of(c * 8, 8), 8)
        weight = tm[part, :].astype(F32) * lax.rsqrt(total / width + 1e-06)
        high = weight.astype(BF16).astype(F32)
        both = jnp.concatenate([high, weight - high], axis=0)
        left = jnp.concatenate([jnp.where(row16 == j, both, 0.0) for j in range(8)], axis=1).astype(BF16)
        sums = jnp.dot(left, tx[pl.ds(c * 8, 8)].reshape(8 * length, feats), preferred_element_type=F32)
        tpool[part, :] = (sums[:8] + sums[8:]) * tg[...].reshape(1, feats)
        return carry

    def pooling(g):
        remote(sqr.at[g], sqr.at[g], sq_send, sq_recv.at[g], partner).wait_recv()
        lax.fori_loop(0, per, functools.partial(pool, g), 0, unroll=True)

    lax.fori_loop(0, per, squares, 0)
    pl.semaphore_wait(barrier, n + dn - 2)
    send_squares(0)
    lax.fori_loop(per, 2 * per, squares, 0)
    send_squares(1)
    spread_mask()
    lax.fori_loop(2 * per, 3 * per, squares, 0)
    send_squares(2)
    lax.fori_loop(3 * per, 4 * per, squares, 0)
    send_squares(3)
    for copy in others:
        copy.start()
    def project(b):
        partial = jnp.dot(tpool[b * span : (b + 1) * span, :].astype(BF16), tp[...], preferred_element_type=F32)
        for j in range(n):
            block = partial[j * rows : (j + 1) * rows]
            pf[b, j] = block
            pb[b, j] = block.astype(BF16)
        for o in range(1, n):
            remote(pb.at[b, lax.rem(me_m + o, n)], pr.at[b, o - 1], rs_send, rs_recv.at[b], mp_peer(o)).start()

    for b in range(parts):
        for g in range(b * GROUPS // parts, (b + 1) * GROUPS // parts):
            pooling(g)
        if b == 0:
            others[0].wait()
        project(b)

    order = nearest(depth)
    peers = side_x * half - 1
    gathered = te.reshape(parts * depth * 2 * side_x * half, rows, embed).at[pl.ds(0, peers)]

    def near(j):
        return choose(me_z, [order[z][j] for z in range(depth)])

    def share(b, z):
        block = te.at[b, z, core, me_x, chip]
        for p in range(peers, 0, -1):
            remote(block, block, plane_send, plane_recv.at[b, z], plane_peer(p)).start()

    def launch(b):
        remote(pr.at[b], pr.at[b], rs_send, rs_recv.at[b], partner).wait_recv()
        summed = pf[b, me_m]
        for o in range(1, n):
            summed = summed + pr[b, o - 1].astype(F32)
        unit = summed * lax.rsqrt(jnp.mean(summed * summed, axis=-1, keepdims=True) + 1e-06) * (embed ** -0.5)
        te[b, me_z, core, me_x, chip] = unit.astype(BF16)
        own = te.at[b, me_z, core, me_x, chip]
        for j in range(depth - 1):
            z = near(depth - 2 - j)
            remote(own, own, z_send, z_recv.at[b, me_z], (z * side_x + me_x, me_m)).start()
        share(b, me_z)

    def pass_on(b, z):
        if peers:
            remote(gathered, gathered, plane_send, plane_recv.at[b, z], partner).wait_recv()
        block = te.at[b, z, core]
        remote(block, block, fw_send, fw_recv.at[b, z], partner).start()

    def relay(b):
        for j in range(depth - 1):
            z = near(j)
            block = te.at[b, z, core, me_x, chip]
            remote(block, block, z_send, z_recv.at[b, z], partner).wait_recv()
            share(b, z)

    others[1].wait()
    gain_col = jnp.transpose(jnp.broadcast_to(sg[...].reshape(1, ds), (LANES, ds)))

    def weigh(k, carry):
        cols = pl.ds(pl.multiple_of(k * LANES, LANES), LANES)
        scaled = (sp[:, cols].astype(F32) * gain_col).astype(BF16)
        sw[k] = scaled
        for j in range(ds // LANES):
            wt_out[j, cols, :] = jnp.transpose(scaled[j * LANES : (j + 1) * LANES])
        return carry

    lax.fori_loop(0, embed // LANES, weigh, 0)
    if parts > 1:
        launch(0)
    others[2].wait()
    stages = ((ua, aa, ca), (ub, ab, cb))
    count = queries // per_tile

    def chunk(c):
        return pl.ds(pl.multiple_of(c * tokens, tokens), tokens)

    tiles = embed // TILE

    def prepare(c, side, k):
        out, _, scale_out = stages[side]
        right = jnp.concatenate([sw[k * (TILE // LANES) + j] for j in range(TILE // LANES)], axis=1)
        out[:, k * TILE : (k + 1) * TILE] = jnp.dot(x_out[chunk(c), :], right, preferred_element_type=F32)

    def rescale(c, side, k):
        scale_out = stages[side][2]
        for r in range(k * tokens // tiles, (k + 1) * tokens // tiles, SLAB):
            part = pl.ds(pl.multiple_of(c * tokens + r, SLAB), SLAB)
            x = x_out[part, :].astype(F32)
            scale = live_col[part, :] * lax.rsqrt(jnp.mean(x * x, axis=-1, keepdims=True) + 1e-06)
            scale_out[r : r + SLAB, :] = scale
            scl_out[part, :] = scale

    group8 = lax.broadcasted_iota(jnp.int32, (2 * per_tile, tokens), 0)
    token8 = lax.broadcasted_iota(jnp.int32, (2 * per_tile, tokens), 1) // qlen
    picks = [jnp.where(group8 == token8 + side * per_tile, 1.0, 0.0).astype(BF16) for side in range(2)]

    def activate(c, side, k):
        held, kept, scale_in = stages[side]
        cols = slice(k * TILE, (k + 1) * TILE)
        for r in range(0, tokens, SLAB):
            u = held[r : r + SLAB, cols] * jnp.concatenate([scale_in[r : r + SLAB, :]] * (TILE // LANES), axis=1)
            z = (u * (ROOT + (ROOT * CUBE) * (u * u))).astype(BF16)
            ul = u.astype(BF16)
            th = jnp.tanh(z)
            part = th * BF16(0.5) + BF16(0.5)
            act = ul * part
            bend = (ul * ul) * BF16(3.0 * ROOT * CUBE) + BF16(ROOT)
            kept[r : r + SLAB, cols] = act
            spot = pl.ds(pl.multiple_of(c * tokens + r, SLAB), SLAB)
            h_out[spot, cols] = part + act * (BF16(1.0) - th) * bend

    def total_up(c, side, k):
        cols = slice(k * TILE, (k + 1) * TILE)
        summed = jnp.dot(picks[side], stages[side][1][:, cols], preferred_element_type=F32)
        spot = pl.ds(pl.multiple_of(c // 2 * (2 * per_tile), 2 * per_tile), 2 * per_tile)
        if side == 0:
            raw_out[spot, cols] = summed
        else:
            raw_out[spot, cols] += summed

    def student(c, carry):
        for side in range(2):

            @pl.when(lax.rem(c, 2) == side)
            def _():
                for k in range(tiles):
                    total_up(jnp.maximum(c - 1, 0), 1 - side, k)
                    rescale(jnp.minimum(c + 1, count - 1), 1 - side, k)
                for k in range(tiles):
                    prepare(jnp.minimum(c + 1, count - 1), 1 - side, k)
                    activate(c, side, k)

        return carry

    ab[...] = jnp.zeros_like(ab)
    raw_out[...] = jnp.zeros_like(raw_out)
    for k in range(tiles):
        prepare(0, 0, k)
        rescale(0, 0, k)
    marks = [count * j // 8 for j in (0, 1, 2, 4, 7, 8)]

    def work(stage):
        lax.fori_loop(marks[stage], marks[stage + 1], student, 0)

    work(0)
    launch(parts - 1)
    work(1)
    if parts > 1:
        relay(0)
    work(2)
    relay(parts - 1)
    if parts > 1:
        pass_on(0, me_z)
    work(3)
    if parts > 1:
        for j in range(depth - 1):
            pass_on(0, near(j))
    work(4)
    for k in range(tiles):
        total_up(count - 1, 1, k)

    raw = raw_out[...]
    scale = lax.rsqrt(jnp.mean(raw * raw, axis=-1, keepdims=True) + 1e-06)
    unit = scale * (embed ** -0.5)
    sround = (raw * unit).astype(BF16)
    total = dn * passages
    place = lax.broadcasted_iota(jnp.int32, (total, queries), 0)
    block, row = place // rows, lax.rem(place, rows)
    piece, block = block // (dn * n), lax.rem(block, dn * n)
    plane, slot = block // (side_x * n), lax.rem(block, side_x * n)
    owner = plane * side_x + lax.rem(slot // half, side_x)
    member = lax.rem(slot, half) * 2 + slot // (half * side_x)
    lines = owner * passages + piece * span + member * rows + row
    picker = jnp.transpose(jnp.where(po[...].reshape(1, queries) == lines, 1.0, 0.0)).astype(BF16)

    pass_on(parts - 1, me_z)
    for j in range(depth - 1):
        pass_on(parts - 1, near(j))
    for b in range(parts):
        for z in range(depth):
            column = te.at[b, z, core]
            remote(column, column, fw_send, fw_recv.at[b, z], partner).wait_recv()
    table = te[...].reshape(total, embed)
    tpos = jnp.dot(picker, table, preferred_element_type=F32).astype(BF16)
    both = jnp.concatenate([tpos, sround], axis=0)
    logits = lax.dot_general(both, table, NT, preferred_element_type=F32)
    texp = jnp.exp(10.0 * logits[:queries])
    sexp = jnp.exp(20.0 * logits[queries:])
    diff = sexp / jnp.sum(sexp, axis=1, keepdims=True) - texp / jnp.sum(texp, axis=1, keepdims=True)
    ge = 20.0 * jnp.dot(diff.astype(BF16), table, preferred_element_type=F32)
    ge_out[...] = ge
    inner = jnp.mean(raw * ge, axis=-1, keepdims=True)
    grad_out[...] = unit * (ge - raw * (scale * scale * inner))
    remote(sqr, sqr, sq_send, sq_recv.at[0], partner).wait_send()
    remote(pr, pr, rs_send, rs_recv.at[0], partner).wait_send()
    sent = te.at[:, pl.ds(0, depth - 1), 0, 0, 0]
    remote(sent, sent, z_send, z_recv.at[0, 0], partner).wait_send()
    if peers:
        for j in range(parts * depth):
            remote(gathered, gathered, plane_send, plane_recv.at[0, 0], partner).wait_send()
    sent = te.at[:, :, 0]
    remote(sent, sent, fw_send, fw_recv.at[0, 0], partner).wait_send()


def back(ge, grad, h, xs, scl, wt, embed_out, states_out, ga, gb, staged, embed_sem, sem):
    total, embed = h.shape
    ds = xs.shape[1]
    queries = grad.shape[0]
    qlen = total // queries
    tokens = TILE
    count = total // tokens
    per_tile = tokens // qlen
    keep = pltpu.make_async_copy(ge, embed_out, embed_sem)
    keep.start()

    def chunk(c):
        return pl.ds(pl.multiple_of(c * tokens, tokens), tokens)

    def store(c):
        return pltpu.make_async_copy(staged.at[chunk(c)], states_out.at[chunk(c)], sem.at[c])

    def multiply(c, out):
        pieces = []
        for j in range(per_tile):
            line = jnp.broadcast_to(grad[pl.ds(c * per_tile + j, 1), :], (16, embed)).astype(BF16)
            part = pl.ds(pl.multiple_of(c * tokens + j * qlen, qlen), qlen)
            pieces.append(h[part, :] * jnp.concatenate([line] * (qlen // 16), axis=0))
        left = jnp.concatenate(pieces, axis=0)
        for k in range(ds // TILE):
            right = jnp.concatenate([wt[k * (TILE // LANES) + j] for j in range(TILE // LANES)], axis=1)
            out[:, k * TILE : (k + 1) * TILE] = jnp.dot(left, right, preferred_element_type=F32)

    def finish(c, held):
        gy = held[...]
        x = xs[chunk(c), :].astype(F32)
        scale = scl[chunk(c), :]
        inner = jnp.mean(x * gy, axis=-1, keepdims=True)
        bias = scale * scale * inner
        wide = lambda v: jnp.concatenate([v] * (ds // LANES), axis=1)
        staged[chunk(c), :] = (wide(scale) * (gy - x * wide(bias))).astype(BF16)
        store(c).start()

    multiply(0, ga)

    def body(i, carry):
        multiply(2 * i + 1, gb)
        finish(2 * i, ga)
        multiply(2 * i + 2, ga)
        finish(2 * i + 1, gb)
        return carry

    lax.fori_loop(0, count // 2 - 1, body, 0, unroll=True)
    multiply(count - 1, gb)
    finish(count - 2, ga)
    finish(count - 1, gb)
    keep.wait()
    for c in range(count):
        store(c).wait()


def shards(dn, n, ts, tgain, tproj, tmask, ss, sgain, sproj, smask, positive):
    passages, length, feats = ts.shape
    embed = tproj.shape[1]
    queries, qlen, ds = ss.shape
    parts = halves_of(passages, n)
    rows = passages // (n * parts)
    total = queries * qlen
    chunks = passages // 8
    side_x = 2 if dn % 2 == 0 else 1
    flat = ss.reshape(total, ds)
    hbm = pl.BlockSpec(memory_space=pltpu.HBM)
    vmem = pl.BlockSpec(memory_space=pltpu.VMEM)
    dma = pltpu.SemaphoreType.DMA
    ge, grad, h, xs, scl, wt = pl.pallas_call(
        functools.partial(front, dn, n),
        out_shape=(
            pltpu.VMEM((queries, embed), F32),
            pltpu.VMEM((queries, embed), F32),
            pltpu.VMEM((total, embed), BF16),
            pltpu.VMEM((total, ds), BF16),
            pltpu.VMEM((total, LANES), F32),
            pltpu.VMEM((ds // LANES, embed, LANES), BF16),
        ),
        in_specs=[hbm] * 9,
        out_specs=(vmem,) * 6,
        scratch_shapes=[
            pltpu.VMEM((passages, length, feats), BF16),
            pltpu.VMEM((feats, embed), BF16),
            pltpu.VMEM((ds, embed), BF16),
            pltpu.VMEM((embed // LANES, ds, LANES), BF16),
            pltpu.VMEM((passages, length), jnp.int32),
            pltpu.VMEM((feats,), F32),
            pltpu.VMEM((ds,), F32),
            pltpu.VMEM((queries, qlen), jnp.int32),
            pltpu.VMEM((queries,), jnp.int32),
            pltpu.VMEM((total, LANES), F32),
            pltpu.VMEM((chunks, 8, length), F32),
            pltpu.VMEM((GROUPS, n - 1, chunks // GROUPS, 8, length), F32),
            pltpu.VMEM((passages, feats), F32),
            pltpu.VMEM((parts, n, rows, embed), F32),
            pltpu.VMEM((parts, n, rows, embed), BF16),
            pltpu.VMEM((parts, n - 1, rows, embed), BF16),
            pltpu.VMEM((parts, dn // side_x, 2, side_x, n // 2, rows, embed), BF16),
            pltpu.VMEM((queries, embed), F32),
            pltpu.VMEM((TILE, embed), F32),
            pltpu.VMEM((TILE, embed), F32),
            pltpu.VMEM((TILE, embed), BF16),
            pltpu.VMEM((TILE, embed), BF16),
            pltpu.VMEM((TILE, LANES), F32),
            pltpu.VMEM((TILE, LANES), F32),
            dma((min(AHEAD, chunks),)),
            dma((8,)),
            dma,
            dma((GROUPS,)),
            dma,
            dma((parts,)),
            dma,
            dma((parts, dn // side_x)),
            dma,
            dma((parts, dn // side_x)),
            dma,
            dma((parts, dn // side_x)),
        ],
        compiler_params=pltpu.CompilerParams(
            collective_id=0, has_side_effects=True, vmem_limit_bytes=56_600_000
        ),
        name="front",
    )(ts, tmask, tgain, tproj, flat, sgain, sproj, smask, positive)
    grad_embed, grad_states = pl.pallas_call(
        back,
        out_shape=(jax.ShapeDtypeStruct((queries, embed), F32), jax.ShapeDtypeStruct((total, ds), BF16)),
        in_specs=[vmem] * 6,
        out_specs=(hbm, hbm),
        scratch_shapes=[
            pltpu.VMEM((TILE, ds), F32),
            pltpu.VMEM((TILE, ds), F32),
            pltpu.VMEM((total, ds), BF16),
            dma,
            dma((total // TILE,)),
        ],
        compiler_params=pltpu.CompilerParams(vmem_limit_bytes=16 * 1024 * 1024),
        name="back",
    )(ge, grad, h, xs, scl, wt)
    return grad_embed, grad_states.reshape(queries, qlen, ds)


def solution(mesh):
    in_specs = (
        P("dp", None, "mp"),
        P("mp"),
        P("mp", None),
        P("dp", None),
        P(("dp", "mp"), None, None),
        P(),
        P(),
        P(("dp", "mp"), None),
        P(("dp", "mp")),
    )
    out_specs = (P(("dp", "mp"), None), P(("dp", "mp"), None, None))
    body = functools.partial(shards, mesh.shape["dp"], mesh.shape["mp"])
    return jax.shard_map(body, mesh=mesh, in_specs=in_specs, out_specs=out_specs, check_vma=False)
```

```python
import functools

import jax
import jax.numpy as jnp
from jax import lax
from jax.experimental import pallas as pl
from jax.experimental.pallas import tpu as pltpu
from jax.sharding import PartitionSpec as P

MESH = pl.DeviceIdType.MESH
F32 = jnp.float32
BF16 = jnp.bfloat16
GROUPS = 4
AHEAD = 5
ROOT = 0.7978845608028654
CUBE = 0.044715
LANES = 128
TILE = 256
SLAB = 16
NT = (((1,), (1,)), ((), ()))


def nearest(count):
    return [sorted(range(count), key=lambda other: abs(other - here))[1:] for here in range(count)]


def halves_of(passages, n):
    return 2 if passages // n % 16 == 0 else 1


def choose(index, values):
    picked = values[0]
    for i, value in enumerate(values[1:], 1):
        picked = jnp.where(index == i, value, picked)
    return picked


def front(
    dn, n, ts, tmask, tgain, tproj, ss, sgain, sproj, smask, pos,
    ge_out, grad_out, h_out, x_out, scl_out, wt_out,
    tx, tp, sp, sw, tm, tg, sg, sm, po, live_col, sq, sqr, tpool, pf, pb, pr, te, wanted, raw_out, ua, ub, aa, ab, ca, cb,
    sem_tx, sem_in, sq_send, sq_recv, rs_send, rs_recv, z_send, z_recv, plane_send, plane_recv, fw_send, fw_recv,
):
    passages, length, feats = tx.shape
    width = n * feats
    parts = halves_of(passages, n)
    rows = passages // (n * parts)
    span = passages // parts
    embed = tp.shape[1]
    chunks = passages // 8
    queries, qlen = sm.shape
    ds = sp.shape[0]
    tokens = TILE
    per_tile = tokens // qlen
    me_d, me_m = lax.axis_index("dp"), lax.axis_index("mp")
    half = n // 2
    core, chip = lax.rem(me_m, 2), me_m // 2

    def mp_peer(o):
        return (me_d, lax.rem(me_m + o, n))

    def dp_peer(o):
        return (lax.rem(me_d + o, dn), me_m)

    side_x = 2 if dn % 2 == 0 else 1
    depth = dn // side_x
    me_z, me_x = me_d // side_x, lax.rem(me_d, side_x)

    def plane_peer(p):
        x = lax.rem(me_x + p // half, side_x)
        return (me_z * side_x + x, 2 * lax.rem(chip + p % half, half) + core)

    partner = (me_d, me_m + 1 - 2 * core)

    def load(c):
        part = pl.ds(c * 8, 8)
        return pltpu.make_async_copy(ts.at[part], tx.at[part], sem_tx.at[lax.rem(c, ahead)])

    ahead = min(AHEAD, chunks)
    moves = [(smask, sm), (tmask, tm), (tgain, tg), (sgain, sg), (pos, po), (tproj, tp), (sproj, sp), (ss, x_out)]
    copies = [pltpu.make_async_copy(a, b, sem_in.at[i]) for i, (a, b) in enumerate(moves)]
    small, others = copies[:5], copies[5:]
    for copy in small:
        copy.start()
    for c in range(ahead):
        load(c).start()
    barrier = pltpu.get_barrier_semaphore()
    for o in range(1, n):
        pl.semaphore_signal(barrier, inc=1, device_id=mp_peer(o), device_id_type=MESH)
    for o in range(1, dn):
        pl.semaphore_signal(barrier, inc=1, device_id=dp_peer(o), device_id_type=MESH)

    def remote(src, dst, send, recv, peer):
        return pltpu.make_async_remote_copy(
            src_ref=src, dst_ref=dst, send_sem=send, recv_sem=recv, device_id=peer, device_id_type=MESH
        )

    def spread_mask():
        for copy in small:
            copy.wait()
        turned = jnp.transpose(sm[...].astype(F32))
        for q in range(queries):
            live_col[q * qlen : (q + 1) * qlen, :] = jnp.broadcast_to(turned[:, q : q + 1], (qlen, LANES))

    ones = jnp.ones((16, TILE), BF16)
    row8 = lax.broadcasted_iota(jnp.int32, (8, length), 0)
    row16 = lax.rem(lax.broadcasted_iota(jnp.int32, (16, length), 0), 8)
    per = chunks // GROUPS

    def squares(c, carry):
        load(c).wait()

        @pl.when(c + ahead < chunks)
        def _():
            load(c + ahead).start()

        held = jnp.zeros((8, length), F32)
        for j in range(8):
            terms = []
            for k in range(feats // TILE):
                x = tx[c * 8 + j, :, k * TILE : (k + 1) * TILE]
                terms.append(x * x)
            while len(terms) > 1:
                terms = [a + b for a, b in zip(terms[::2], terms[1::2])] + terms[len(terms) // 2 * 2 :]
            line = lax.dot_general(ones, terms[0], NT, preferred_element_type=F32)
            held = jnp.where(row8 == j, line[:8], held)
        sq[c] = held
        return carry

    def send_squares(g):
        part = pl.ds(g * per, per)
        for o in range(1, n):
            remote(sq.at[part], sqr.at[g, o - 1], sq_send, sq_recv.at[g], mp_peer(o)).start()

    def pool(g, i, carry):
        c = g * per + i
        total = sq[c]
        for o in range(1, n):
            total = total + sqr[g, o - 1, i]
        part = pl.ds(pl.multiple_of(c * 8, 8), 8)
        weight = tm[part, :].astype(F32) * lax.rsqrt(total / width + 1e-06)
        high = weight.astype(BF16).astype(F32)
        both = jnp.concatenate([high, weight - high], axis=0)
        left = jnp.concatenate([jnp.where(row16 == j, both, 0.0) for j in range(8)], axis=1).astype(BF16)
        sums = jnp.dot(left, tx[pl.ds(c * 8, 8)].reshape(8 * length, feats), preferred_element_type=F32)
        tpool[part, :] = (sums[:8] + sums[8:]) * tg[...].reshape(1, feats)
        return carry

    def pooling(g):
        remote(sqr.at[g], sqr.at[g], sq_send, sq_recv.at[g], partner).wait_recv()
        lax.fori_loop(0, per, functools.partial(pool, g), 0, unroll=True)

    lax.fori_loop(0, per, squares, 0)
    pl.semaphore_wait(barrier, n + dn - 2)
    send_squares(0)
    lax.fori_loop(per, 2 * per, squares, 0)
    send_squares(1)
    spread_mask()
    lax.fori_loop(2 * per, 3 * per, squares, 0)
    send_squares(2)
    lax.fori_loop(3 * per, 4 * per, squares, 0)
    send_squares(3)
    for copy in others:
        copy.start()
    def project(b):
        partial = jnp.dot(tpool[b * span : (b + 1) * span, :].astype(BF16), tp[...], preferred_element_type=F32)
        for j in range(n):
            block = partial[j * rows : (j + 1) * rows]
            pf[b, j] = block
            pb[b, j] = block.astype(BF16)
        for o in range(1, n):
            remote(pb.at[b, lax.rem(me_m + o, n)], pr.at[b, o - 1], rs_send, rs_recv.at[b], mp_peer(o)).start()

    for b in range(parts):
        for g in range(b * GROUPS // parts, (b + 1) * GROUPS // parts):
            pooling(g)
        if b == 0:
            others[0].wait()
        project(b)

    order = nearest(depth)
    peers = side_x * half - 1
    gathered = te.reshape(parts * depth * 2 * side_x * half, rows, embed).at[pl.ds(0, peers)]

    def near(j):
        return choose(me_z, [order[z][j] for z in range(depth)])

    def share(b, z):
        block = te.at[b, z, core, me_x, chip]
        for p in range(peers, 0, -1):
            remote(block, block, plane_send, plane_recv.at[b, z], plane_peer(p)).start()

    def launch(b):
        remote(pr.at[b], pr.at[b], rs_send, rs_recv.at[b], partner).wait_recv()
        summed = pf[b, me_m]
        for o in range(1, n):
            summed = summed + pr[b, o - 1].astype(F32)
        unit = summed * lax.rsqrt(jnp.mean(summed * summed, axis=-1, keepdims=True) + 1e-06) * (embed ** -0.5)
        te[b, me_z, core, me_x, chip] = unit.astype(BF16)
        own = te.at[b, me_z, core, me_x, chip]
        for j in range(depth - 1):
            z = near(depth - 2 - j)
            remote(own, own, z_send, z_recv.at[b, me_z], (z * side_x + me_x, me_m)).start()
        share(b, me_z)

    def pass_on(b, z):
        if peers:
            remote(gathered, gathered, plane_send, plane_recv.at[b, z], partner).wait_recv()
        block = te.at[b, z, core]
        remote(block, block, fw_send, fw_recv.at[b, z], partner).start()

    def relay(b):
        for j in range(depth - 1):
            z = near(j)
            block = te.at[b, z, core, me_x, chip]
            remote(block, block, z_send, z_recv.at[b, z], partner).wait_recv()
            share(b, z)

    others[1].wait()
    gain_col = jnp.transpose(jnp.broadcast_to(sg[...].reshape(1, ds), (LANES, ds)))

    def weigh(k, carry):
        cols = pl.ds(pl.multiple_of(k * LANES, LANES), LANES)
        scaled = (sp[:, cols].astype(F32) * gain_col).astype(BF16)
        sw[k] = scaled
        for j in range(ds // LANES):
            wt_out[j, cols, :] = jnp.transpose(scaled[j * LANES : (j + 1) * LANES])
        return carry

    lax.fori_loop(0, embed // LANES, weigh, 0)
    if parts > 1:
        launch(0)
    others[2].wait()
    stages = ((ua, aa, ca), (ub, ab, cb))
    count = queries // per_tile

    def chunk(c):
        return pl.ds(pl.multiple_of(c * tokens, tokens), tokens)

    tiles = embed // TILE

    def prepare(c, side, k):
        out, _, scale_out = stages[side]
        right = jnp.concatenate([sw[k * (TILE // LANES) + j] for j in range(TILE // LANES)], axis=1)
        out[:, k * TILE : (k + 1) * TILE] = jnp.dot(x_out[chunk(c), :], right, preferred_element_type=F32)

    def rescale(c, side, k):
        scale_out = stages[side][2]
        for r in range(k * tokens // tiles, (k + 1) * tokens // tiles, SLAB):
            part = pl.ds(pl.multiple_of(c * tokens + r, SLAB), SLAB)
            x = x_out[part, :].astype(F32)
            scale = live_col[part, :] * lax.rsqrt(jnp.mean(x * x, axis=-1, keepdims=True) + 1e-06)
            scale_out[r : r + SLAB, :] = scale
            scl_out[part, :] = scale

    group8 = lax.broadcasted_iota(jnp.int32, (2 * per_tile, tokens), 0)
    token8 = lax.broadcasted_iota(jnp.int32, (2 * per_tile, tokens), 1) // qlen
    picks = [jnp.where(group8 == token8 + side * per_tile, 1.0, 0.0).astype(BF16) for side in range(2)]

    def activate(c, side, k):
        held, kept, scale_in = stages[side]
        cols = slice(k * TILE, (k + 1) * TILE)
        for r in range(0, tokens, SLAB):
            u = held[r : r + SLAB, cols] * jnp.concatenate([scale_in[r : r + SLAB, :]] * (TILE // LANES), axis=1)
            z = (u * (ROOT + (ROOT * CUBE) * (u * u))).astype(BF16)
            ul = u.astype(BF16)
            th = jnp.tanh(z)
            part = th * BF16(0.5) + BF16(0.5)
            act = ul * part
            bend = (ul * ul) * BF16(3.0 * ROOT * CUBE) + BF16(ROOT)
            kept[r : r + SLAB, cols] = act
            spot = pl.ds(pl.multiple_of(c * tokens + r, SLAB), SLAB)
            h_out[spot, cols] = part + act * (BF16(1.0) - th) * bend

    def total_up(c, side, k):
        cols = slice(k * TILE, (k + 1) * TILE)
        summed = jnp.dot(picks[side], stages[side][1][:, cols], preferred_element_type=F32)
        spot = pl.ds(pl.multiple_of(c // 2 * (2 * per_tile), 2 * per_tile), 2 * per_tile)
        if side == 0:
            raw_out[spot, cols] = summed
        else:
            raw_out[spot, cols] += summed

    def student(c, carry):
        for side in range(2):

            @pl.when(lax.rem(c, 2) == side)
            def _():
                for k in range(tiles):
                    total_up(jnp.maximum(c - 1, 0), 1 - side, k)
                    rescale(jnp.minimum(c + 1, count - 1), 1 - side, k)
                for k in range(tiles):
                    prepare(jnp.minimum(c + 1, count - 1), 1 - side, k)
                    activate(c, side, k)

        return carry

    ab[...] = jnp.zeros_like(ab)
    raw_out[...] = jnp.zeros_like(raw_out)
    for k in range(tiles):
        prepare(0, 0, k)
        rescale(0, 0, k)
    marks = [count * j // 8 for j in (0, 1, 3, 4, 7, 8)]

    def work(stage):
        lax.fori_loop(marks[stage], marks[stage + 1], student, 0)

    work(0)
    launch(parts - 1)
    work(1)
    total = dn * passages
    place = lax.broadcasted_iota(jnp.int32, (total, queries), 0)
    block, row = place // rows, lax.rem(place, rows)
    piece, block = block // (dn * n), lax.rem(block, dn * n)
    plane, slot = block // (side_x * n), lax.rem(block, side_x * n)
    owner = plane * side_x + lax.rem(slot // half, side_x)
    member = lax.rem(slot, half) * 2 + slot // (half * side_x)
    lines = owner * passages + piece * span + member * rows + row
    wanted[...] = jnp.transpose(jnp.where(po[...].reshape(1, queries) == lines, 1.0, 0.0)).astype(BF16)
    if parts > 1:
        relay(0)
    work(2)
    relay(parts - 1)
    if parts > 1:
        pass_on(0, me_z)
    work(3)
    if parts > 1:
        for j in range(depth - 1):
            pass_on(0, near(j))
    pass_on(parts - 1, me_z)
    work(4)
    pass_on(parts - 1, near(0))
    for k in range(tiles):
        total_up(count - 1, 1, k)

    raw = raw_out[...]
    scale = lax.rsqrt(jnp.mean(raw * raw, axis=-1, keepdims=True) + 1e-06)
    unit = scale * (embed ** -0.5)
    sround = (raw * unit).astype(BF16)
    for j in range(1, depth - 1):
        pass_on(parts - 1, near(j))
    for b in range(parts):
        for z in range(depth):
            column = te.at[b, z, core]
            remote(column, column, fw_send, fw_recv.at[b, z], partner).wait_recv()
    table = te[...].reshape(total, embed)
    tpos = jnp.dot(wanted[...], table, preferred_element_type=F32).astype(BF16)
    both = jnp.concatenate([tpos, sround], axis=0)
    logits = lax.dot_general(both, table, NT, preferred_element_type=F32)
    texp = jnp.exp(10.0 * logits[:queries])
    sexp = jnp.exp(20.0 * logits[queries:])
    diff = sexp / jnp.sum(sexp, axis=1, keepdims=True) - texp / jnp.sum(texp, axis=1, keepdims=True)
    ge = 20.0 * jnp.dot(diff.astype(BF16), table, preferred_element_type=F32)
    ge_out[...] = ge
    inner = jnp.mean(raw * ge, axis=-1, keepdims=True)
    grad_out[...] = unit * (ge - raw * (scale * scale * inner))
    remote(sqr, sqr, sq_send, sq_recv.at[0], partner).wait_send()
    remote(pr, pr, rs_send, rs_recv.at[0], partner).wait_send()
    sent = te.at[:, pl.ds(0, depth - 1), 0, 0, 0]
    remote(sent, sent, z_send, z_recv.at[0, 0], partner).wait_send()
    if peers:
        for j in range(parts * depth):
            remote(gathered, gathered, plane_send, plane_recv.at[0, 0], partner).wait_send()
    sent = te.at[:, :, 0]
    remote(sent, sent, fw_send, fw_recv.at[0, 0], partner).wait_send()


def back(ge, grad, h, xs, scl, wt, embed_out, states_out, ga, gb, staged, embed_sem, sem):
    total, embed = h.shape
    ds = xs.shape[1]
    queries = grad.shape[0]
    qlen = total // queries
    tokens = TILE
    count = total // tokens
    per_tile = tokens // qlen
    keep = pltpu.make_async_copy(ge, embed_out, embed_sem)
    keep.start()

    def chunk(c):
        return pl.ds(pl.multiple_of(c * tokens, tokens), tokens)

    def store(c):
        return pltpu.make_async_copy(staged.at[chunk(c)], states_out.at[chunk(c)], sem.at[c])

    def multiply(c, out):
        pieces = []
        for j in range(per_tile):
            line = jnp.broadcast_to(grad[pl.ds(c * per_tile + j, 1), :], (16, embed)).astype(BF16)
            part = pl.ds(pl.multiple_of(c * tokens + j * qlen, qlen), qlen)
            pieces.append(h[part, :] * jnp.concatenate([line] * (qlen // 16), axis=0))
        left = jnp.concatenate(pieces, axis=0)
        for k in range(ds // TILE):
            right = jnp.concatenate([wt[k * (TILE // LANES) + j] for j in range(TILE // LANES)], axis=1)
            out[:, k * TILE : (k + 1) * TILE] = jnp.dot(left, right, preferred_element_type=F32)

    def finish(c, held):
        gy = held[...]
        x = xs[chunk(c), :].astype(F32)
        scale = scl[chunk(c), :]
        inner = jnp.mean(x * gy, axis=-1, keepdims=True)
        bias = scale * scale * inner
        wide = lambda v: jnp.concatenate([v] * (ds // LANES), axis=1)
        staged[chunk(c), :] = (wide(scale) * (gy - x * wide(bias))).astype(BF16)
        store(c).start()

    multiply(0, ga)

    def body(i, carry):
        multiply(2 * i + 1, gb)
        finish(2 * i, ga)
        multiply(2 * i + 2, ga)
        finish(2 * i + 1, gb)
        return carry

    lax.fori_loop(0, count // 2 - 1, body, 0, unroll=True)
    multiply(count - 1, gb)
    finish(count - 2, ga)
    finish(count - 1, gb)
    keep.wait()
    for c in range(count):
        store(c).wait()


def shards(dn, n, ts, tgain, tproj, tmask, ss, sgain, sproj, smask, positive):
    passages, length, feats = ts.shape
    embed = tproj.shape[1]
    queries, qlen, ds = ss.shape
    parts = halves_of(passages, n)
    rows = passages // (n * parts)
    total = queries * qlen
    chunks = passages // 8
    side_x = 2 if dn % 2 == 0 else 1
    flat = ss.reshape(total, ds)
    hbm = pl.BlockSpec(memory_space=pltpu.HBM)
    vmem = pl.BlockSpec(memory_space=pltpu.VMEM)
    dma = pltpu.SemaphoreType.DMA
    ge, grad, h, xs, scl, wt = pl.pallas_call(
        functools.partial(front, dn, n),
        out_shape=(
            pltpu.VMEM((queries, embed), F32),
            pltpu.VMEM((queries, embed), F32),
            pltpu.VMEM((total, embed), BF16),
            pltpu.VMEM((total, ds), BF16),
            pltpu.VMEM((total, LANES), F32),
            pltpu.VMEM((ds // LANES, embed, LANES), BF16),
        ),
        in_specs=[hbm] * 9,
        out_specs=(vmem,) * 6,
        scratch_shapes=[
            pltpu.VMEM((passages, length, feats), BF16),
            pltpu.VMEM((feats, embed), BF16),
            pltpu.VMEM((ds, embed), BF16),
            pltpu.VMEM((embed // LANES, ds, LANES), BF16),
            pltpu.VMEM((passages, length), jnp.int32),
            pltpu.VMEM((feats,), F32),
            pltpu.VMEM((ds,), F32),
            pltpu.VMEM((queries, qlen), jnp.int32),
            pltpu.VMEM((queries,), jnp.int32),
            pltpu.VMEM((total, LANES), F32),
            pltpu.VMEM((chunks, 8, length), F32),
            pltpu.VMEM((GROUPS, n - 1, chunks // GROUPS, 8, length), F32),
            pltpu.VMEM((passages, feats), F32),
            pltpu.VMEM((parts, n, rows, embed), F32),
            pltpu.VMEM((parts, n, rows, embed), BF16),
            pltpu.VMEM((parts, n - 1, rows, embed), BF16),
            pltpu.VMEM((parts, dn // side_x, 2, side_x, n // 2, rows, embed), BF16),
            pltpu.VMEM((queries, dn * passages), BF16),
            pltpu.VMEM((queries, embed), F32),
            pltpu.VMEM((TILE, embed), F32),
            pltpu.VMEM((TILE, embed), F32),
            pltpu.VMEM((TILE, embed), BF16),
            pltpu.VMEM((TILE, embed), BF16),
            pltpu.VMEM((TILE, LANES), F32),
            pltpu.VMEM((TILE, LANES), F32),
            dma((min(AHEAD, chunks),)),
            dma((8,)),
            dma,
            dma((GROUPS,)),
            dma,
            dma((parts,)),
            dma,
            dma((parts, dn // side_x)),
            dma,
            dma((parts, dn // side_x)),
            dma,
            dma((parts, dn // side_x)),
        ],
        compiler_params=pltpu.CompilerParams(
            collective_id=0, has_side_effects=True, vmem_limit_bytes=56_600_000
        ),
        name="front",
    )(ts, tmask, tgain, tproj, flat, sgain, sproj, smask, positive)
    grad_embed, grad_states = pl.pallas_call(
        back,
        out_shape=(jax.ShapeDtypeStruct((queries, embed), F32), jax.ShapeDtypeStruct((total, ds), BF16)),
        in_specs=[vmem] * 6,
        out_specs=(hbm, hbm),
        scratch_shapes=[
            pltpu.VMEM((TILE, ds), F32),
            pltpu.VMEM((TILE, ds), F32),
            pltpu.VMEM((total, ds), BF16),
            dma,
            dma((total // TILE,)),
        ],
        compiler_params=pltpu.CompilerParams(vmem_limit_bytes=16 * 1024 * 1024),
        name="back",
    )(ge, grad, h, xs, scl, wt)
    return grad_embed, grad_states.reshape(queries, qlen, ds)


def solution(mesh):
    in_specs = (
        P("dp", None, "mp"),
        P("mp"),
        P("mp", None),
        P("dp", None),
        P(("dp", "mp"), None, None),
        P(),
        P(),
        P(("dp", "mp"), None),
        P(("dp", "mp")),
    )
    out_specs = (P(("dp", "mp"), None), P(("dp", "mp"), None, None))
    body = functools.partial(shards, mesh.shape["dp"], mesh.shape["mp"])
    return jax.shard_map(body, mesh=mesh, in_specs=in_specs, out_specs=out_specs, check_vma=False)
```
